32 devices in a mesh: group: 4 (over y, x), shard: 8 (over z, core).
Axes of the slice: x: 2, y: 2, z: 4, core: 2. Of those that a mesh axis runs over, the one named last changes fastest.
Arguments:
- amplitudes: float32 [32768, 128], P(('group', 'shard')), may hold values from -6 to 6
- orbit_index: int32 [32768, 128], P(('group', 'shard')), may hold values from 0 to 5
- requests: int32 [32, 32, 2], P(('group', 'shard')), may hold values from 0 to 1024, as said below
- targets: int32 [32, 32, 2], P(('group', 'shard')), may hold values from 0 to 1023
Outputs:
- image: float32 [32768, 128], P(('group', 'shard'))
The draws below stay inside these ranges and needn't reach their ends.
Inputs may be any that keep to these rules, and one draw needn't show every extreme that they name: `requests`: each value is an owner's local block number below 1024, or 1024 for an empty slot; in every list from one requester to one owner the used slots come first; every draw has owners whose lists from every requester are full (2 blocks).
All inputs are finite; a program needn't handle non-finite values.
Results may differ from the reference program's by a relative error of at most 0.0003.
Values sent between devices are 32-bit elements; how exact they have to be, the bound alone decides.
A program may use at most 64 MiB of HBM per device.

```python
import jax
import jax.numpy as jnp
from jax import lax

NB = 1024
BLK = 128
CAP = 2
RANKS = 32
TOTAL_BLOCKS = 32768


def draw_requests(key, part):
    first, second, third = jax.random.split(key, 3)
    counts = jax.random.randint(first, (RANKS, RANKS), max(1, CAP // 2), CAP + 1)
    popular = jax.random.randint(second, (4,), 0, RANKS)
    is_popular = jnp.any(jnp.arange(RANKS)[:, None] == popular[None, :], axis=1)
    counts = jnp.where(is_popular[None, :], CAP, counts)
    numbers = jax.random.randint(third, (RANKS, RANKS, CAP), 0, NB)
    slots = jnp.arange(CAP)
    return jnp.where(slots[None, None, :] < counts[:, :, None], numbers, NB).astype(jnp.int32)


def place_ends(array, stream_key, smallest, top_value):
    shape = array.shape
    spot = [jax.random.randint(jax.random.fold_in(stream_key, axis), (), 0, shape[axis]) for axis in range(len(shape))]
    array = array.at[tuple(spot)].set(smallest)
    longest = shape.index(max(shape))
    spot[longest] = (spot[longest] + 1) % shape[longest]
    return array.at[tuple(spot)].set(top_value)


def block_levels(key, dims, cuts, least, high):
    loudness = 1.0
    for dim, parts in cuts:
        heights = jax.random.uniform(jax.random.fold_in(jax.random.fold_in(key, 6), dim), (parts,), jnp.float32, least / len(cuts), high / len(cuts))
        loudness = loudness * jnp.repeat(jnp.exp(heights), dims[dim] // parts).reshape((-1,) + (1,) * (len(dims) - 1 - dim))
    return loudness


def centred(rng, extent, width, bound, shards=(), held_as=jnp.bfloat16):
    factor_of = block_levels(rng, extent, shards, -0.22, 0.18) if shards else 1.0
    array = jax.random.normal(rng, extent, jnp.float32) * width * factor_of
    return jnp.minimum(jnp.maximum(array, -bound), bound).astype(held_as)


def setup_inputs(seed: int = 0) -> dict:
    key_list = jax.random.split(jax.random.key(seed), 5)
    return {
        "amplitudes": centred(key_list[0], (TOTAL_BLOCKS, BLK), 1.0, 6.0, ((0, 32),), jnp.float32),
        "orbit_index": place_ends(jax.random.randint(key_list[1], (TOTAL_BLOCKS, BLK), 0, 6), jax.random.fold_in(key_list[1], 1), 0, 5).astype(jnp.int32),
        "requests": draw_requests(jax.random.fold_in(key_list[4], 71), 0),
        "targets": place_ends(jax.random.randint(key_list[3], (RANKS, RANKS, CAP), 0, NB), jax.random.fold_in(key_list[3], 1), 0, NB - 1).astype(jnp.int32),
    }


def reference(amplitudes, orbit_index, requests, targets):
    factor = jnp.sqrt(96.0 * jnp.exp2(-orbit_index.astype(amplitudes.dtype)))
    weighted = amplitudes * factor
    total = weighted.shape[0]
    lanes = weighted.shape[1]
    padded = jnp.concatenate([weighted, jnp.zeros((1, lanes), weighted.dtype)], axis=0)
    owners = jnp.arange(RANKS, dtype=jnp.int32)

    def visit(totals, requester):
        wanted = requests[requester]
        valid = wanted < NB
        global_rows = jnp.where(valid, owners[:, None] * NB + wanted, total).astype(jnp.int32).reshape(-1)
        places = (requester * NB + targets[requester]).astype(jnp.int32).reshape(-1)
        fetched = padded[global_rows]
        totals = totals.at[places].add(fetched)
        totals = totals.at[global_rows].add(weighted[places])
        return (totals, None)
    start = jnp.zeros((total + 1, lanes), weighted.dtype)
    totals, unused = lax.scan(visit, start, jnp.arange(RANKS, dtype=jnp.int32))
    return totals[:total] / factor
```

```python
import functools

import jax
import jax.numpy as jnp
from jax import lax
from jax.experimental import pallas as pl
from jax.experimental.pallas import tpu as pltpu
from jax.sharding import PartitionSpec as P

MESH = pl.DeviceIdType.MESH


def split(x):
    hi = x.astype(jnp.bfloat16)
    lo = (x - hi.astype(jnp.float32)).astype(jnp.bfloat16)
    return jnp.concatenate([hi, lo], axis=1)


def kernel(groups, shards, cap, req_hbm, tgt_hbm, amp_hbm, orb_hbm, out_ref,
           req, tgt, amp, orb, inv, halves, onehot, ids_out, rows_out, back_out, ids_in, rows_in,
           load_sem, ids_send, ids_recv, rows_send, rows_recv, back_send, back_recv):
    ranks = groups * shards
    slots = ranks * cap
    blocks, lanes = amp.shape
    me_g, me_s = lax.axis_index("group"), lax.axis_index("shard")
    me = me_g * shards + me_s

    loads = [
        pltpu.make_async_copy(src, dst, load_sem.at[i])
        for i, (src, dst) in enumerate(((req_hbm, req), (tgt_hbm, tgt), (amp_hbm, amp), (orb_hbm, orb)))
    ]
    for load in loads:
        load.start()

    def peer(k):
        rank = lax.rem(me + k, ranks)
        return rank, (lax.div(rank, shards), lax.rem(rank, shards))

    barrier = pltpu.get_barrier_semaphore()

    def greet(k, carry):
        pl.semaphore_signal(barrier, inc=1, device_id=peer(k)[1], device_id_type=MESH)
        return carry

    lax.fori_loop(1, ranks, greet, 0)

    loads[0].wait()
    loads[1].wait()

    def spread(o, carry):
        for c in range(cap):
            ids_out[o, c:c + 1, :] = jnp.full((1, lanes), req[0, c, o], jnp.int32)
            ids_in[ranks + o, c:c + 1, :] = jnp.full((1, lanes), tgt[0, c, o], jnp.int32)
        return carry

    lax.fori_loop(0, ranks, spread, 0, unroll=4)
    ids_in[me] = ids_out[me]
    pl.semaphore_wait(barrier, ranks - 1)

    def exchange(src, dst, base, send_sem, recv_sem):
        def body(k, carry):
            rank, device = peer(k)
            pltpu.make_async_remote_copy(
                src_ref=src.at[rank], dst_ref=dst.at[base + me], send_sem=send_sem, recv_sem=recv_sem,
                device_id=device, device_id_type=MESH,
            ).start()
            return carry

        lax.fori_loop(1, ranks, body, 0)

    def wait_all(ref, sem):
        part = ref.at[pl.ds(0, ranks - 1)]
        pltpu.make_async_copy(part, part, sem).wait()

    exchange(ids_out, ids_in, 0, ids_send, ids_recv)
    loads[2].wait()
    loads[3].wait()
    level = orb[...].astype(jnp.float32)
    factor = jnp.sqrt(96.0 * jnp.exp2(-level))
    halves[...] = split(amp[...] * factor)
    inv[...] = 1.0 / factor

    def gather(ids):
        place = lax.broadcasted_iota(jnp.int32, (slots, blocks), 1)
        wanted = jnp.concatenate([ids] * (blocks // lanes), axis=1)
        picks = jnp.where(place == wanted, 1.0, 0.0).astype(jnp.bfloat16)
        both = jnp.dot(picks, halves[...], preferred_element_type=jnp.float32)
        return (both[:, :lanes] + both[:, lanes:]).reshape(ranks, cap, lanes)

    rows_out[...] = gather(ids_in[ranks:].reshape(slots, lanes))
    rows_in[me] = rows_out[me]
    exchange(rows_out, rows_in, 0, rows_send, rows_recv)

    wait_all(ids_in, ids_recv)
    back_out[...] = gather(ids_in[:ranks].reshape(slots, lanes))
    rows_in[ranks + me] = back_out[me]
    exchange(back_out, rows_in, ranks, back_send, back_recv)

    ids = ids_in[...].reshape(2 * slots, lanes)
    for start in range(0, 2 * slots, lanes):
        part = ids[start:start + lanes]
        diagonal = lax.broadcasted_iota(jnp.int32, (lanes, lanes), 0) == lax.broadcasted_iota(
            jnp.int32, (lanes, lanes), 1
        )
        line = jnp.sum(jnp.where(diagonal, part, 0), axis=0, keepdims=True)
        place = lax.broadcasted_iota(jnp.int32, (blocks, lanes), 0)
        onehot[:, start:start + lanes] = jnp.where(place == line, 1.0, 0.0).astype(jnp.bfloat16)

    wait_all(rows_in, rows_recv)
    wait_all(rows_in, back_recv)
    rows = split(rows_in[...].reshape(2 * slots, lanes))
    both = jnp.dot(onehot[...], rows, preferred_element_type=jnp.float32)
    out_ref[...] = (both[:, :lanes] + both[:, lanes:]) * inv[...]
    wait_all(ids_out, ids_send)
    wait_all(rows_out, rows_send)
    wait_all(back_out, back_send)


def per_device(amplitudes, orbit_index, requests, targets):
    groups = lax.axis_size("group")
    shards = lax.axis_size("shard")
    ranks = groups * shards
    cap = requests.shape[-1]
    blocks, lanes = amplitudes.shape
    slot_rows = (ranks, cap, lanes)
    both_rows = (2 * ranks, cap, lanes)
    anywhere = pl.BlockSpec(memory_space=pl.ANY)
    return pl.pallas_call(
        functools.partial(kernel, groups, shards, cap),
        out_shape=jax.ShapeDtypeStruct((blocks, lanes), jnp.float32),
        in_specs=[anywhere] * 4,
        out_specs=pl.BlockSpec(memory_space=pltpu.VMEM),
        scratch_shapes=[
            pltpu.SMEM((1, cap, ranks), jnp.int32),
            pltpu.SMEM((1, cap, ranks), jnp.int32),
            pltpu.VMEM((blocks, lanes), jnp.float32),
            pltpu.VMEM((blocks, lanes), jnp.int32),
            pltpu.VMEM((blocks, lanes), jnp.float32),
            pltpu.VMEM((blocks, 2 * lanes), jnp.bfloat16),
            pltpu.VMEM((blocks, 2 * ranks * cap), jnp.bfloat16),
            pltpu.VMEM(slot_rows, jnp.int32),
            pltpu.VMEM(slot_rows, jnp.float32),
            pltpu.VMEM(slot_rows, jnp.float32),
            pltpu.VMEM(both_rows, jnp.int32),
            pltpu.VMEM(both_rows, jnp.float32),
            pltpu.SemaphoreType.DMA((4,)),
        ] + [pltpu.SemaphoreType.DMA] * 6,
        compiler_params=pltpu.CompilerParams(collective_id=0, has_side_effects=True),
        name="couple",
    )(requests.transpose(0, 2, 1), targets.transpose(0, 2, 1), amplitudes, orbit_index)


def solution(mesh):
    return jax.shard_map(
        per_device,
        mesh=mesh,
        in_specs=(
            P(("group", "shard"), None),
            P(("group", "shard"), None),
            P(("group", "shard"), None, None),
            P(("group", "shard"), None, None),
        ),
        out_specs=P(("group", "shard"), None),
        check_vma=False,
    )
```

```python
import functools

import jax
import jax.numpy as jnp
from jax import lax
from jax.experimental import pallas as pl
from jax.experimental.pallas import tpu as pltpu
from jax.sharding import PartitionSpec as P

MESH = pl.DeviceIdType.MESH


def split(x):
    hi = x.astype(jnp.bfloat16)
    lo = (x - hi.astype(jnp.float32)).astype(jnp.bfloat16)
    return jnp.concatenate([hi, lo], axis=1)


def kernel(groups, shards, cap, req_hbm, tgt_hbm, amp_hbm, orb_hbm, out_ref,
           req, tgt, amp, orb, inv, halves, onehot, ids_out, rows_out, back_out, ids_in, rows_in,
           load_sem, ids_send, ids_recv, rows_send, rows_recv, back_send, back_recv):
    ranks = groups * shards
    slots = ranks * cap
    blocks, lanes = amp.shape
    me_g, me_s = lax.axis_index("group"), lax.axis_index("shard")
    me = me_g * shards + me_s

    upper = (me >= ranks // 2).astype(jnp.int32)
    mirror = upper * me + (1 - upper) * (ranks - 1 - me)

    def peer(k):
        skipped = k + (k >= mirror).astype(jnp.int32)
        rank = upper * skipped + (1 - upper) * (ranks - 1 - skipped)
        return rank, (rank // shards, rank % shards)

    barrier = pltpu.get_barrier_semaphore()

    def greet(k, carry):
        pl.semaphore_signal(barrier, inc=1, device_id=peer(k)[1], device_id_type=MESH)
        return carry

    lax.fori_loop(0, ranks - 1, greet, 0)

    loads = [
        pltpu.make_async_copy(src, dst, load_sem.at[i])
        for i, (src, dst) in enumerate(((req_hbm, req), (tgt_hbm, tgt), (amp_hbm, amp), (orb_hbm, orb)))
    ]
    for load in loads:
        load.start()

    loads[0].wait()
    loads[1].wait()

    def spread(o, carry):
        for c in range(cap):
            ids_out[o, c:c + 1, :] = jnp.full((1, lanes), req[0, c, o], jnp.int32)
            ids_in[ranks + o, c:c + 1, :] = jnp.full((1, lanes), tgt[0, c, o], jnp.int32)
        return carry

    lax.fori_loop(0, ranks, spread, 0, unroll=4)
    ids_in[me] = ids_out[me]
    pl.semaphore_wait(barrier, ranks - 1)

    def exchange(src, dst, base, send_sem, recv_sem):
        def body(k, carry):
            rank, device = peer(k)
            pltpu.make_async_remote_copy(
                src_ref=src.at[rank], dst_ref=dst.at[base + me], send_sem=send_sem, recv_sem=recv_sem,
                device_id=device, device_id_type=MESH,
            ).start()
            return carry

        lax.fori_loop(0, ranks - 1, body, 0)

    def wait_all(ref, sem):
        part = ref.at[pl.ds(0, ranks - 1)]
        pltpu.make_async_copy(part, part, sem).wait()

    exchange(ids_out, ids_in, 0, ids_send, ids_recv)
    loads[2].wait()
    loads[3].wait()
    level = orb[...].astype(jnp.float32)
    factor = jnp.sqrt(96.0 * jnp.exp2(-level))
    halves[...] = split(amp[...] * factor)
    inv[...] = 1.0 / factor

    def gather(ids):
        place = lax.broadcasted_iota(jnp.int32, (slots, blocks), 1)
        wanted = jnp.concatenate([ids] * (blocks // lanes), axis=1)
        picks = jnp.where(place == wanted, 1.0, 0.0).astype(jnp.bfloat16)
        both = jnp.dot(picks, halves[...], preferred_element_type=jnp.float32)
        return (both[:, :lanes] + both[:, lanes:]).reshape(ranks, cap, lanes)

    rows_out[...] = gather(ids_in[ranks:].reshape(slots, lanes))
    rows_in[me] = rows_out[me]
    exchange(rows_out, rows_in, 0, rows_send, rows_recv)

    wait_all(ids_in, ids_recv)
    back_out[...] = gather(ids_in[:ranks].reshape(slots, lanes))
    rows_in[ranks + me] = back_out[me]
    exchange(back_out, rows_in, ranks, back_send, back_recv)

    ids = ids_in[...].reshape(2 * slots, lanes)
    for start in range(0, 2 * slots, lanes):
        part = ids[start:start + lanes]
        diagonal = lax.broadcasted_iota(jnp.int32, (lanes, lanes), 0) == lax.broadcasted_iota(
            jnp.int32, (lanes, lanes), 1
        )
        line = jnp.sum(jnp.where(diagonal, part, 0), axis=0, keepdims=True)
        place = lax.broadcasted_iota(jnp.int32, (blocks, lanes), 0)
        onehot[:, start:start + lanes] = jnp.where(place == line, 1.0, 0.0).astype(jnp.bfloat16)

    wait_all(rows_in, rows_recv)
    wait_all(rows_in, back_recv)
    rows = split(rows_in[...].reshape(2 * slots, lanes))
    both = jnp.dot(onehot[...], rows, preferred_element_type=jnp.float32)
    out_ref[...] = (both[:, :lanes] + both[:, lanes:]) * inv[...]
    wait_all(ids_out, ids_send)
    wait_all(rows_out, rows_send)
    wait_all(back_out, back_send)


def per_device(amplitudes, orbit_index, requests, targets):
    groups = lax.axis_size("group")
    shards = lax.axis_size("shard")
    ranks = groups * shards
    cap = requests.shape[-1]
    blocks, lanes = amplitudes.shape
    slot_rows = (ranks, cap, lanes)
    both_rows = (2 * ranks, cap, lanes)
    anywhere = pl.BlockSpec(memory_space=pltpu.HBM)
    return pl.pallas_call(
        functools.partial(kernel, groups, shards, cap),
        out_shape=jax.ShapeDtypeStruct((blocks, lanes), jnp.float32),
        in_specs=[anywhere] * 4,
        out_specs=pl.BlockSpec(memory_space=pltpu.VMEM),
        scratch_shapes=[
            pltpu.SMEM((1, cap, ranks), jnp.int32),
            pltpu.SMEM((1, cap, ranks), jnp.int32),
            pltpu.VMEM((blocks, lanes), jnp.float32),
            pltpu.VMEM((blocks, lanes), jnp.int32),
            pltpu.VMEM((blocks, lanes), jnp.float32),
            pltpu.VMEM((blocks, 2 * lanes), jnp.bfloat16),
            pltpu.VMEM((blocks, 2 * ranks * cap), jnp.bfloat16),
            pltpu.VMEM(slot_rows, jnp.int32),
            pltpu.VMEM(slot_rows, jnp.float32),
            pltpu.VMEM(slot_rows, jnp.float32),
            pltpu.VMEM(both_rows, jnp.int32),
            pltpu.VMEM(both_rows, jnp.float32),
            pltpu.SemaphoreType.DMA((4,)),
        ] + [pltpu.SemaphoreType.DMA] * 6,
        compiler_params=pltpu.CompilerParams(collective_id=0, has_side_effects=True, vmem_limit_bytes=32*1024*1024),
        name="couple",
    )(*(pltpu.with_memory_space_constraint(x, pltpu.HBM) for x in (requests.transpose(0, 2, 1), targets.transpose(0, 2, 1), amplitudes, orbit_index)))


def solution(mesh):
    return jax.shard_map(
        per_device,
        mesh=mesh,
        in_specs=(
            P(("group", "shard"), None),
            P(("group", "shard"), None),
            P(("group", "shard"), None, None),
            P(("group", "shard"), None, None),
        ),
        out_specs=P(("group", "shard"), None),
        check_vma=False,
    )
```

```python
import functools

import jax
import jax.numpy as jnp
from jax import lax
from jax.experimental import pallas as pl
from jax.experimental.pallas import tpu as pltpu
from jax.sharding import PartitionSpec as P

MESH = pl.DeviceIdType.MESH


def split(x):
    hi = x.astype(jnp.bfloat16)
    lo = (x - hi.astype(jnp.float32)).astype(jnp.bfloat16)
    return jnp.concatenate([hi, lo], axis=1)


def kernel(groups, shards, cap, req_hbm, tgt_hbm, amp_hbm, orb_hbm, out_ref,
           req, tgt, amp, orb, inv, halves, onehot, ids_out, rows_out, back_out, ids_in, rows_in,
           load_sem, ids_send, ids_recv, rows_send, rows_recv, back_send, back_recv):
    ranks = groups * shards
    slots = ranks * cap
    blocks, lanes = amp.shape
    me_g, me_s = lax.axis_index("group"), lax.axis_index("shard")
    me = me_g * shards + me_s

    upper = (me >= ranks // 2).astype(jnp.int32)
    mirror = upper * me + (1 - upper) * (ranks - 1 - me)

    def peer(k):
        skipped = k + (k >= mirror).astype(jnp.int32)
        rank = upper * skipped + (1 - upper) * (ranks - 1 - skipped)
        return rank, (rank // shards, rank % shards)

    barrier = pltpu.get_barrier_semaphore()

    def greet(k, carry):
        pl.semaphore_signal(barrier, inc=1, device_id=peer(k)[1], device_id_type=MESH)
        return carry

    lax.fori_loop(0, ranks - 1, greet, 0, unroll=4)

    loads = [
        pltpu.make_async_copy(src, dst, load_sem.at[i])
        for i, (src, dst) in enumerate(((req_hbm, req), (tgt_hbm, tgt), (amp_hbm, amp), (orb_hbm, orb)))
    ]
    for load in loads:
        load.start()

    loads[0].wait()
    loads[1].wait()

    def spread(o, carry):
        for c in range(cap):
            ids_out[o, c:c + 1, :] = jnp.full((1, lanes), req[0, c, o], jnp.int32)
            ids_in[ranks + o, c:c + 1, :] = jnp.full((1, lanes), tgt[0, c, o], jnp.int32)
        return carry

    lax.fori_loop(0, ranks, spread, 0, unroll=4)
    ids_in[me] = ids_out[me]
    pl.semaphore_wait(barrier, ranks - 1)

    def exchange(src, dst, base, send_sem, recv_sem):
        def body(k, carry):
            rank, device = peer(k)
            pltpu.make_async_remote_copy(
                src_ref=src.at[rank], dst_ref=dst.at[base + me], send_sem=send_sem, recv_sem=recv_sem,
                device_id=device, device_id_type=MESH,
            ).start()
            return carry

        lax.fori_loop(0, ranks - 1, body, 0, unroll=4)

    def wait_all(ref, sem):
        part = ref.at[pl.ds(0, ranks - 1)]
        pltpu.make_async_copy(part, part, sem).wait()

    exchange(ids_out, ids_in, 0, ids_send, ids_recv)
    loads[2].wait()
    loads[3].wait()
    level = orb[...].astype(jnp.float32)
    factor = jnp.sqrt(96.0 * jnp.exp2(-level))
    halves[...] = split(amp[...] * factor)
    inv[...] = 1.0 / factor

    def gather(ids):
        place = lax.broadcasted_iota(jnp.int32, (slots, blocks), 1)
        wanted = jnp.concatenate([ids] * (blocks // lanes), axis=1)
        picks = jnp.where(place == wanted, 1.0, 0.0).astype(jnp.bfloat16)
        both = jnp.dot(picks, halves[...], preferred_element_type=jnp.float32)
        return (both[:, :lanes] + both[:, lanes:]).reshape(ranks, cap, lanes)

    rows_out[...] = gather(ids_in[ranks:].reshape(slots, lanes))
    rows_in[me] = rows_out[me]
    exchange(rows_out, rows_in, 0, rows_send, rows_recv)

    wait_all(ids_in, ids_recv)
    back_out[...] = gather(ids_in[:ranks].reshape(slots, lanes))
    rows_in[ranks + me] = back_out[me]
    exchange(back_out, rows_in, ranks, back_send, back_recv)

    ids = ids_in[...].reshape(2 * slots, lanes)
    for start in range(0, 2 * slots, lanes):
        part = ids[start:start + lanes]
        diagonal = lax.broadcasted_iota(jnp.int32, (lanes, lanes), 0) == lax.broadcasted_iota(
            jnp.int32, (lanes, lanes), 1
        )
        line = jnp.sum(jnp.where(diagonal, part, 0), axis=0, keepdims=True)
        place = lax.broadcasted_iota(jnp.int32, (blocks, lanes), 0)
        onehot[:, start:start + lanes] = jnp.where(place == line, 1.0, 0.0).astype(jnp.bfloat16)

    wait_all(rows_in, rows_recv)
    wait_all(rows_in, back_recv)
    rows = split(rows_in[...].reshape(2 * slots, lanes))
    both = jnp.dot(onehot[...], rows, preferred_element_type=jnp.float32)
    out_ref[...] = (both[:, :lanes] + both[:, lanes:]) * inv[...]
    wait_all(ids_out, ids_send)
    wait_all(rows_out, rows_send)
    wait_all(back_out, back_send)


def per_device(amplitudes, orbit_index, requests, targets):
    groups = lax.axis_size("group")
    shards = lax.axis_size("shard")
    ranks = groups * shards
    cap = requests.shape[-1]
    blocks, lanes = amplitudes.shape
    slot_rows = (ranks, cap, lanes)
    both_rows = (2 * ranks, cap, lanes)
    anywhere = pl.BlockSpec(memory_space=pltpu.HBM)
    return pl.pallas_call(
        functools.partial(kernel, groups, shards, cap),
        out_shape=jax.ShapeDtypeStruct((blocks, lanes), jnp.float32),
        in_specs=[anywhere] * 4,
        out_specs=pl.BlockSpec(memory_space=pltpu.VMEM),
        scratch_shapes=[
            pltpu.SMEM((1, cap, ranks), jnp.int32),
            pltpu.SMEM((1, cap, ranks), jnp.int32),
            pltpu.VMEM((blocks, lanes), jnp.float32),
            pltpu.VMEM((blocks, lanes), jnp.int32),
            pltpu.VMEM((blocks, lanes), jnp.float32),
            pltpu.VMEM((blocks, 2 * lanes), jnp.bfloat16),
            pltpu.VMEM((blocks, 2 * ranks * cap), jnp.bfloat16),
            pltpu.VMEM(slot_rows, jnp.int32),
            pltpu.VMEM(slot_rows, jnp.float32),
            pltpu.VMEM(slot_rows, jnp.float32),
            pltpu.VMEM(both_rows, jnp.int32),
            pltpu.VMEM(both_rows, jnp.float32),
            pltpu.SemaphoreType.DMA((4,)),
        ] + [pltpu.SemaphoreType.DMA] * 6,
        compiler_params=pltpu.CompilerParams(collective_id=0, has_side_effects=True, vmem_limit_bytes=32*1024*1024),
        name="couple",
    )(*(pltpu.with_memory_space_constraint(x, pltpu.HBM) for x in (requests.transpose(0, 2, 1), targets.transpose(0, 2, 1), amplitudes, orbit_index)))


def solution(mesh):
    return jax.shard_map(
        per_device,
        mesh=mesh,
        in_specs=(
            P(("group", "shard"), None),
            P(("group", "shard"), None),
            P(("group", "shard"), None, None),
            P(("group", "shard"), None, None),
        ),
        out_specs=P(("group", "shard"), None),
        check_vma=False,
    )
```
